32 devices in a mesh: chan: 4 (over x, core), bl: 8 (over z, y).
Axes of the slice: x: 2, y: 2, z: 4, core: 2. Of those that a mesh axis runs over, the one named last changes fastest.
Arguments:
- vis_value: bfloat16 [4, 8, 2, 2048], P('chan', 'bl'), may hold values from -6 to 6
- vis_weight: bfloat16 [4, 8, 2048], P('chan', 'bl'), may hold values from 0.19921875 to 5
- kernel: bfloat16 [4, 8, 64, 2048], P('chan', 'bl'), may hold values from 0.049804688 to 1
- tile_index: int32 [4, 8, 2048], P('chan', 'bl'), may hold values from 0 to 262143
- plane_index: int32 [4, 8, 2048], P('chan', 'bl'), may hold values from 0 to 7
- chan_index: int32 [4, 8, 2048], P('chan', 'bl'), may hold values from 0 to 15
- chan_offset: float32 [4, 16], P('chan'), may hold values from -0.4 to 0.4
- counts: int32 [4, 8], P('chan', 'bl'), may hold values from 256 to 2048, as said below
Outputs:
- taylor_coeffs: float32 [3, 32768], P(None, ('chan', 'bl'))
The draws below stay inside these ranges and needn't reach their ends.
Inputs may be any that keep to these rules, and one draw needn't show every extreme that they name: `counts`: each device's number of live visibility slots; slots from that number on are ignored. In every draw some device has exactly 2048.
All inputs are finite; a program needn't handle non-finite values.
Results may differ from the reference program's by a relative error of at most 0.0003.
Values may be sent and summed in bfloat16 or wider, within the bound.
A program may use at most 128 MiB of HBM per device.

```python
import math
import jax
import jax.numpy as jnp
from jax import lax

NPIX = 4096
TILE = 8
NTILE = 512
TAYLOR = 3
MOMENTS = 5
WPLANES = 8
CH_DEV = 16
STRIP = 8
SLOTS = 2048
BLK = 256
N_CHAN = 4
N_BL = 8


def draw_counts(key, part):
    raw = jax.random.randint(jax.random.fold_in(key, 11), (N_CHAN, N_BL), 0, 1000)
    spread = raw * raw // 1000 * (SLOTS - BLK) // 1000
    base_counts = (BLK + spread).reshape(-1)
    chosen = jax.random.randint(jax.random.fold_in(key, 12), (), 0, N_CHAN * N_BL)
    filled = jnp.where(jnp.arange(N_CHAN * N_BL) == chosen, SLOTS, base_counts)
    return filled.reshape(N_CHAN, N_BL).astype(jnp.int32)


def place_ends(values, key, least, high):
    dims = values.shape
    index_at = [jax.random.randint(jax.random.fold_in(key, axis), (), 0, dims[axis]) for axis in range(len(dims))]
    values = values.at[tuple(index_at)].set(least)
    longest = dims.index(max(dims))
    index_at[longest] = (index_at[longest] + 1) % dims[longest]
    return values.at[tuple(index_at)].set(high)


def block_levels(stream_key, dims, pieces, least, top_value):
    def one(axis_at, shards_of):
        draws = jax.random.uniform(jax.random.fold_in(jax.random.fold_in(stream_key, 6), axis_at), (shards_of,), jnp.float32, least / len(pieces), top_value / len(pieces))
        return jnp.repeat(jnp.exp(draws), dims[axis_at] // shards_of).reshape((-1,) + (1,) * (len(dims) - axis_at - 1))

    gain = one(*pieces[0])
    for cut in pieces[1:]:
        gain = gain * one(*cut)
    return gain


def scatter_about(stream_key, shape, width, limit, cuts=(), kind=jnp.bfloat16):
    result = jax.random.normal(stream_key, shape, jnp.float32) * width
    if len(cuts) > 0:
        result = block_levels(stream_key, shape, cuts, -0.22, 0.18) * result
    return jnp.clip(result, min=-limit, max=limit).astype(kind)


def setup_inputs(seed: int = 0) -> dict:
    arg_keys = jax.random.split(jax.random.key(seed), 9)
    vis_value = scatter_about(arg_keys[0], (N_CHAN, N_BL, 2, SLOTS), 1.0, 6.0, ((0, 4), (1, 8)))
    vis_weight = jnp.clip(jnp.exp(math.log(5.0) - 3.2227897 * jax.random.uniform(arg_keys[1], (N_CHAN, N_BL, SLOTS), jnp.float32) ** block_levels(arg_keys[1], (N_CHAN, N_BL, SLOTS), ((0, 4), (1, 8)), -0.2, 0.2)), 0.19921875, 5.0).astype(jnp.bfloat16)
    kernel = jnp.clip(0.049804688 + 0.9501953 * jax.random.uniform(arg_keys[2], (N_CHAN, N_BL, TILE * TILE, SLOTS), jnp.float32) ** block_levels(arg_keys[2], (N_CHAN, N_BL, TILE * TILE, SLOTS), ((0, 4), (1, 8)), -0.2, 0.2), 0.049804688, 1.0).astype(jnp.bfloat16)
    tile_index = place_ends(jax.random.randint(arg_keys[3], (N_CHAN, N_BL, SLOTS), 0, NTILE * NTILE), jax.random.fold_in(arg_keys[3], 1), 0, (NTILE * NTILE) - 1).astype(jnp.int32)
    plane_index = place_ends(jax.random.randint(arg_keys[4], (N_CHAN, N_BL, SLOTS), 0, WPLANES), jax.random.fold_in(arg_keys[4], 1), 0, WPLANES - 1).astype(jnp.int32)
    chan_index = place_ends(jax.random.randint(arg_keys[5], (N_CHAN, N_BL, SLOTS), 0, CH_DEV), jax.random.fold_in(arg_keys[5], 1), 0, CH_DEV - 1).astype(jnp.int32)
    chan_offset = jnp.clip(jax.random.uniform(arg_keys[6], (N_CHAN, CH_DEV), jnp.float32, -0.4, 0.4) * block_levels(arg_keys[6], (N_CHAN, CH_DEV), ((0, 4),), -0.4, 0.0), -0.4, 0.4)
    counts = draw_counts(jax.random.fold_in(arg_keys[8], 71), 0)
    return dict(vis_value=vis_value, vis_weight=vis_weight, kernel=kernel, tile_index=tile_index, plane_index=plane_index, chan_index=chan_index, chan_offset=chan_offset, counts=counts)


two_pi = 6.283185307179586
w_step = 40.0

def device_terms(values, weights, kernel, tiles, planes, chans, offsets, live_count):
    slot_count = weights.shape[0]
    ntiles = NPIX // TILE
    live_mask = jnp.arange(slot_count, dtype=jnp.int32) < live_count
    channel_ids = jnp.arange(CH_DEV, dtype=jnp.int32)
    taylor_coord = lax.optimization_barrier(jnp.sum(jnp.where(chans[:, None] == channel_ids[None, :], offsets[None, :], 0.0), axis=1))
    live_weight = jnp.where(live_mask, weights.astype(jnp.float32), 0.0)
    kernel_taps = kernel.astype(jnp.float32).reshape(TILE, TILE, slot_count)
    strip_rows = jnp.arange(STRIP, dtype=jnp.int32) - STRIP // 2
    grid_cols = (tiles // ntiles)[:, None] * TILE + jnp.arange(TILE, dtype=jnp.int32)[None, :] - NPIX // 2
    phase_index = grid_cols[:, :, None] * strip_rows[None, None, :] % NPIX
    phase_angle = phase_index.astype(jnp.float32) * (two_pi / NPIX)
    tile_real = jnp.einsum('abj,jal->jlb', kernel_taps, jnp.cos(phase_angle), precision=lax.Precision.HIGHEST)
    tile_imag = jnp.einsum('abj,jal->jlb', kernel_taps, jnp.sin(phase_angle), precision=lax.Precision.HIGHEST)
    base_real = live_weight * values[0].astype(jnp.float32)
    base_imag = live_weight * values[1].astype(jnp.float32)
    power_list = [jnp.ones_like(taylor_coord)]
    for power_id in range(MOMENTS - 1):
        power_list.append(power_list[power_id] * taylor_coord)
    power_stack = jnp.stack(power_list[:TAYLOR], axis=1)
    coeff_real = base_real[:, None] * power_stack
    coeff_imag = base_imag[:, None] * power_stack
    part_real = coeff_real[:, :, None, None] * tile_real[:, None] - coeff_imag[:, :, None, None] * tile_imag[:, None]
    part_imag = coeff_real[:, :, None, None] * tile_imag[:, None] + coeff_imag[:, :, None, None] * tile_real[:, None]
    updates = jnp.stack([part_real, part_imag], axis=-1).reshape(slot_count, TAYLOR * STRIP * TILE * 2)
    target_rows = planes * ntiles + tiles % ntiles
    tap_sums = lax.optimization_barrier(jnp.sum(kernel_taps, axis=(0, 1)))
    weighted_taps = live_weight * tap_sums
    moment_add = jnp.stack([jnp.sum(weighted_taps * power_list[moment_id]) for moment_id in range(MOMENTS)])
    return (updates, target_rows, moment_add)

def screen_angle(plane_ids, column_ids):
    cell_size = 0.5 / NPIX
    strip_rows = jnp.arange(STRIP, dtype=jnp.int32) - STRIP // 2
    xcoord = strip_rows.astype(jnp.float32) * cell_size
    ycoord = (column_ids - NPIX // 2).astype(jnp.float32) * cell_size
    radius = xcoord[:, None] * xcoord[:, None] + ycoord[None, :] * ycoord[None, :]
    lowered = -radius / (1.0 + jnp.sqrt(1.0 - radius))
    w_value = w_step * (plane_ids.astype(jnp.float32) - 0.5 * (WPLANES - 1))
    return two_pi * w_value[:, None, None] * lowered[None]

def solve_taylor(moments, images):
    entry_00, entry_01, entry_02 = (moments[0], moments[1], moments[2])
    entry_11, entry_12, entry_22 = (moments[2], moments[3], moments[4])
    minor_00 = entry_11 * entry_22 - entry_12 * entry_12
    minor_01 = entry_02 * entry_12 - entry_01 * entry_22
    minor_02 = entry_01 * entry_12 - entry_02 * entry_11
    minor_11 = entry_00 * entry_22 - entry_02 * entry_02
    minor_12 = entry_01 * entry_02 - entry_00 * entry_12
    minor_22 = entry_00 * entry_11 - entry_01 * entry_01
    determinant = entry_00 * minor_00 + entry_01 * minor_01 + entry_02 * minor_02
    first = (minor_00 * images[0] + minor_01 * images[1] + minor_02 * images[2]) / determinant
    second = (minor_01 * images[0] + minor_11 * images[1] + minor_12 * images[2]) / determinant
    third = (minor_02 * images[0] + minor_12 * images[1] + minor_22 * images[2]) / determinant
    return jnp.stack([first, second, third])

def reference(vis_value, vis_weight, kernel, tile_index, plane_index, chan_index, chan_offset, counts):
    device_total = N_CHAN * N_BL
    slot_count = vis_weight.shape[-1]
    ntiles = NPIX // TILE
    offsets_all = jnp.repeat(chan_offset, N_BL, axis=0)
    inputs = (vis_value.reshape(device_total, 2, slot_count), vis_weight.reshape(device_total, slot_count), kernel.reshape(device_total, TILE * TILE, slot_count), tile_index.reshape(device_total, slot_count), plane_index.reshape(device_total, slot_count), chan_index.reshape(device_total, slot_count), offsets_all, counts.reshape(device_total))

    def accumulate(state_pair, sliced):
        uv_grid, moments = state_pair
        updates, target_rows, moment_add = device_terms(*sliced)
        return ((uv_grid.at[target_rows].add(updates), moments + moment_add), None)
    initial = (jnp.zeros((WPLANES * ntiles, TAYLOR * STRIP * TILE * 2), jnp.float32), jnp.zeros((MOMENTS,), jnp.float32))
    (uv_grid, moments), unused = lax.scan(accumulate, initial, inputs)
    cube = uv_grid.reshape(WPLANES, ntiles, TAYLOR, STRIP, TILE, 2)
    cube = jnp.transpose(cube, (0, 2, 3, 1, 4, 5)).reshape(WPLANES, TAYLOR, STRIP, NPIX, 2)
    column_ids = jnp.arange(NPIX, dtype=jnp.int32)
    parity = 1.0 - 2.0 * (column_ids % 2).astype(jnp.float32)
    spectrum = (cube[..., 0] + 1j * cube[..., 1]) * parity
    transformed = jnp.fft.ifft(spectrum, axis=-1) * NPIX
    angles = screen_angle(jnp.arange(WPLANES, dtype=jnp.int32), column_ids)
    image = lax.optimization_barrier(jnp.sum(parity * (jnp.real(transformed) * jnp.cos(angles)[:, None] - jnp.imag(transformed) * jnp.sin(angles)[:, None]), axis=0))
    return solve_taylor(moments, image.reshape(TAYLOR, STRIP * NPIX))
```

```python
import functools

import numpy as np
import jax
import jax.numpy as jnp
from jax import lax
from jax.experimental import pallas as pl
from jax.experimental.pallas import tpu as pltpu
from jax.sharding import PartitionSpec as P

NPIX = 4096
TILE = 8
TAYLOR = 3
MOMENTS = 5
WPLANES = 8
STRIP = 8
BLK = 256
LANES = 128

two_pi = 2.0 * np.pi
w_step = 40.0
ntiles = NPIX // TILE
radix = 256
fine = NPIX // radix
half = fine * STRIP
MESH = pl.DeviceIdType.MESH


def split(x):
    high = x.astype(jnp.bfloat16)
    low = (x - high.astype(jnp.float32)).astype(jnp.bfloat16)
    return high, low


@functools.cache
def tables():
    f32 = np.float32
    bf16 = jnp.bfloat16

    def two(x):
        x = x.astype(f32)
        high = x.astype(bf16)
        return high, (x - high.astype(f32)).astype(bf16)

    rows = np.arange(STRIP) - STRIP // 2
    taps = np.zeros((2, TILE, STRIP, TILE, TILE))
    angle = two_pi * np.arange(TILE)[:, None] * rows[None, :] / NPIX
    for e in range(TILE):
        taps[0, e, :, :, e] = np.cos(angle).T
        taps[1, e, :, :, e] = np.sin(angle).T
    tap_high, tap_low = two(taps.reshape(2 * TILE * STRIP, TILE * TILE))
    tap_table = np.concatenate([tap_high, tap_low], axis=1)
    ids = np.arange(radix)
    angle = two_pi * (ids[:, None] * ids[None, :] % radix) / radix
    coarse_high, coarse_low = two(np.concatenate([np.cos(angle), np.sin(angle)], axis=1))
    coarse = np.concatenate([coarse_high, coarse_low], axis=0)
    cells = np.arange(fine)
    angle = two_pi * cells[:, None] * ids[None, :] / NPIX
    sign = 1.0 - 2.0 * ((cells[:, None] + ids[None, :]) % 2)
    twist = np.stack([np.cos(angle) * sign, np.sin(angle) * sign])
    twist = np.repeat(twist, STRIP, axis=1).astype(f32)
    angle = two_pi * (cells[:, None] * cells[None, :] % fine) / fine
    eye = np.eye(STRIP)
    cosine = np.einsum("me,lL->lmeL", np.cos(angle), eye).reshape(half, half)
    sine = np.einsum("me,lL->lmeL", np.sin(angle), eye).reshape(half, half)
    fine_high, fine_low = two(np.block([[cosine, -sine], [sine, cosine]]))
    fine_table = np.concatenate([fine_high, fine_low, fine_high], axis=1)
    cell_size = 0.5 / NPIX
    x = rows * cell_size
    y = (np.arange(NPIX) - NPIX // 2) * cell_size
    radius = x[:, None] ** 2 + y[None, :] ** 2
    lowered = -radius / (1.0 + np.sqrt(1.0 - radius))
    w = w_step * (np.arange(WPLANES // 2) - 0.5 * (WPLANES - 1))
    angle = two_pi * w[:, None, None] * lowered[None]
    angle = angle.reshape(WPLANES // 2, STRIP * fine, radix)
    screen = np.stack([np.cos(angle), np.sin(angle)], axis=1).astype(f32)
    return tap_table, coarse, twist, fine_table, screen


def image_kernel(
    count_ref, offset_ref, value_ref, weight_ref, kernel_ref, tile_ref, plane_ref, chan_ref,
    tap_ref, coarse_hbm, twist_hbm, fine_hbm, screen_hbm,
    image_ref, moment_ref, coarse_ref, twist_ref, fine_ref, screen_ref, grid_ref, upd_ref, mom_ref, turn_ref, flat_ref, sems,
):
    loads = [
        pltpu.make_async_copy(source, target, sems.at[i])
        for i, (source, target) in enumerate((
            (coarse_hbm, coarse_ref), (twist_hbm, twist_ref),
            (fine_hbm, fine_ref), (screen_hbm, screen_ref),
        ))
    ]
    for load in loads:
        load.start()
    count = count_ref[0, 0]
    grid_ref[...] = jnp.zeros_like(grid_ref)
    mom_ref[...] = jnp.zeros_like(mom_ref)

    def one_block(block, carry):
        first = pl.multiple_of(block * BLK, BLK)
        here = pl.ds(first, BLK)
        slot = first + lax.broadcasted_iota(jnp.int32, (1, BLK), 1)
        tiles = tile_ref[:, here]
        planes = plane_ref[:, here]
        chans = chan_ref[:, here]
        coord = jnp.zeros((1, BLK), jnp.float32)
        for c in range(offset_ref.shape[1]):
            coord = jnp.where(chans == c, offset_ref[0, c], coord)
        weight = weight_ref[0:1, here].astype(jnp.float32)
        weight = jnp.where(slot < count, weight, 0.0)
        taps = kernel_ref[:, here]
        value = value_ref[:, here].astype(jnp.float32)
        base_real = weight * value[0:1]
        base_imag = weight * value[1:2]

        u_tile = lax.shift_right_logical(tiles, 9)
        v_tile = tiles & (ntiles - 1)
        strip = lax.broadcasted_iota(jnp.int32, (STRIP, BLK), 0) - STRIP // 2
        phase = ((u_tile - ntiles // 2) * strip) & (ntiles - 1)
        angle = phase.astype(jnp.float32) * (two_pi / ntiles)
        cosine = jnp.cos(angle)
        sine = jnp.sin(angle)
        z_real = base_real * cosine - base_imag * sine
        z_imag = base_real * sine + base_imag * cosine

        sums = jnp.dot(
            tap_ref[...], jnp.concatenate([taps, taps], axis=0),
            preferred_element_type=jnp.float32,
        )
        sum_real = sums[: TILE * STRIP].reshape(TILE, STRIP, BLK)
        sum_imag = sums[TILE * STRIP :].reshape(TILE, STRIP, BLK)
        part_real = (sum_real * z_real[None] - sum_imag * z_imag[None]).reshape(-1, BLK)
        part_imag = (sum_real * z_imag[None] + sum_imag * z_real[None]).reshape(-1, BLK)
        odd = (v_tile & 1).astype(jnp.float32)
        even = 1.0 - odd
        for k in range(TAYLOR):
            for c, part in enumerate((part_real, part_imag)):
                for side, mask in enumerate((even, odd)):
                    high, low = split(part * mask)
                    row = (k * 2 + c) * half + side * (half // 2)
                    upd_ref[row : row + half // 2, :BLK] = high
                    upd_ref[row : row + half // 2, BLK:] = low
            if k + 1 < TAYLOR:
                part_real = part_real * coord
                part_imag = part_imag * coord

        weighted = weight * jnp.sum(taps.astype(jnp.float32), axis=0, keepdims=True)
        for m in range(MOMENTS):
            mom_ref[m : m + 1, :] += weighted
            weighted = weighted * coord

        target = planes * radix + lax.shift_right_logical(v_tile, 1)
        column = jnp.transpose(jnp.broadcast_to(target.astype(jnp.float32), (LANES, BLK)))
        column = jnp.concatenate([column, column], axis=1)
        update = upd_ref[...]
        lane = lax.broadcasted_iota(jnp.int32, (BLK, radix), 1).astype(jnp.float32)
        for p in range(WPLANES):
            hot = jnp.where(column == lane + float(p * radix), 1.0, 0.0).astype(jnp.bfloat16)
            grid_ref[p] += jnp.dot(
                update, jnp.concatenate([hot, hot], axis=0),
                preferred_element_type=jnp.float32,
            )
        return carry

    lax.fori_loop(0, (count + BLK - 1) // BLK, one_block, 0)
    moment_ref[...] = jnp.broadcast_to(
        jnp.sum(mom_ref[...], axis=1, keepdims=True), moment_ref.shape
    )

    for load in loads:
        load.wait()
    coarse_high = coarse_ref[:radix]
    coarse_table = jnp.concatenate([coarse_high, coarse_ref[radix:], coarse_high], axis=0)
    turn_ref[...] = jnp.zeros_like(turn_ref)

    def one_plane(p, carry):
        high, low = split(grid_ref[p])
        spectra = jnp.dot(
            jnp.concatenate([high, high, low], axis=1), coarse_table,
            preferred_element_type=jnp.float32,
        )
        mirror = jnp.minimum(p, WPLANES - 1 - p)
        sign = jnp.where(p < WPLANES // 2, 1.0, -1.0)
        screen_real = screen_ref[mirror, 0]
        screen_imag = screen_ref[mirror, 1] * sign
        for k in range(TAYLOR):
            real = spectra[2 * k * half : (2 * k + 1) * half]
            imag = spectra[(2 * k + 1) * half : (2 * k + 2) * half]
            f_real = real[:, :radix] - imag[:, radix:]
            f_imag = imag[:, :radix] + real[:, radix:]
            x_real = f_real * twist_ref[0] - f_imag * twist_ref[1]
            x_imag = f_real * twist_ref[1] + f_imag * twist_ref[0]
            x_high, x_low = split(jnp.concatenate([x_real, x_imag], axis=0))
            y = jnp.dot(
                fine_ref[...], jnp.concatenate([x_high, x_high, x_low], axis=0),
                preferred_element_type=jnp.float32,
            )
            turn_ref[k] += y[:half] * screen_real - y[half:] * screen_imag
        return carry

    lax.fori_loop(0, WPLANES, one_plane, 0)
    pieces = radix // LANES
    chunks, _, rows, _ = image_ref.shape
    for k in range(TAYLOR):
        for h in range(pieces):
            flat_ref[pl.ds(h, half, stride=pieces), :] = turn_ref[k, :, h * LANES : (h + 1) * LANES]
        image_ref[:, k] = flat_ref[...].reshape(chunks, rows, LANES)


def local_image(chunks, count, offsets, value, weight, kernel, tiles, planes, chans):
    rows = STRIP * NPIX // (chunks * LANES)
    consts = [jnp.asarray(t) for t in tables()]
    smem = pl.BlockSpec(memory_space=pltpu.SMEM)
    vmem = pl.BlockSpec(memory_space=pltpu.VMEM)
    hbm = pl.BlockSpec(memory_space=pl.ANY)
    columns = 2 * TAYLOR * half
    return pl.pallas_call(
        image_kernel,
        out_shape=(
            jax.ShapeDtypeStruct((chunks, TAYLOR, rows, LANES), jnp.float32),
            jax.ShapeDtypeStruct((8, LANES), jnp.float32),
        ),
        in_specs=[smem, smem] + [vmem] * 7 + [hbm] * 4,
        out_specs=(vmem, vmem),
        scratch_shapes=[pltpu.VMEM(c.shape, c.dtype) for c in consts[1:]]
        + [
            pltpu.VMEM((WPLANES, columns, radix), jnp.float32),
            pltpu.VMEM((columns, 2 * BLK), jnp.bfloat16),
            pltpu.VMEM((8, BLK), jnp.float32),
            pltpu.VMEM((TAYLOR, half, radix), jnp.float32),
            pltpu.VMEM((half * radix // LANES, LANES), jnp.float32),
            pltpu.SemaphoreType.DMA((4,)),
        ],
        compiler_params=pltpu.CompilerParams(vmem_limit_bytes=56 * 1024 * 1024),
        name="local_image",
    )(count, offsets, value, weight, kernel, tiles, planes, chans, *consts)


def solve_taylor(moments, images):
    entry_00, entry_01, entry_02 = (moments[0], moments[1], moments[2])
    entry_11, entry_12, entry_22 = (moments[2], moments[3], moments[4])
    minor_00 = entry_11 * entry_22 - entry_12 * entry_12
    minor_01 = entry_02 * entry_12 - entry_01 * entry_22
    minor_02 = entry_01 * entry_12 - entry_02 * entry_11
    minor_11 = entry_00 * entry_22 - entry_02 * entry_02
    minor_12 = entry_01 * entry_02 - entry_00 * entry_12
    minor_22 = entry_00 * entry_11 - entry_01 * entry_01
    determinant = entry_00 * minor_00 + entry_01 * minor_01 + entry_02 * minor_02
    first = (minor_00 * images[0] + minor_01 * images[1] + minor_02 * images[2]) / determinant
    second = (minor_01 * images[0] + minor_11 * images[1] + minor_12 * images[2]) / determinant
    third = (minor_02 * images[0] + minor_12 * images[1] + minor_22 * images[2]) / determinant
    return first, second, third


def reduce_kernel(
    n_chan, n_bl, image_ref, moment_ref, out_ref,
    work_ref, land_ref, sum_ref, mom_send_ref, mom_land_ref, bl_land_ref, bl_mom_ref,
    send_sem, recv_sem, mom_send_sem, mom_recv_sem, bl_send, bl_recv, blm_send, blm_recv,
):
    chan = lax.axis_index("chan")
    bl = lax.axis_index("bl")
    steps = n_chan.bit_length() - 1

    def partner(s):
        return chan + (1 - 2 * ((chan // 2**s) % 2)) * 2**s

    def peer(d):
        return lax.rem(bl + d, n_bl)

    barrier = pltpu.get_barrier_semaphore()
    for s in range(steps):
        pl.semaphore_signal(barrier, inc=1, device_id=(partner(s), bl), device_id_type=MESH)
    for d in range(1, n_bl):
        pl.semaphore_signal(barrier, inc=1, device_id=(chan, peer(d)), device_id_type=MESH)
    pl.semaphore_wait(barrier, steps + n_bl - 1)

    slot = 0
    for s in range(steps):
        stride = 2 ** (s + 1)
        pieces = n_chan // stride
        copies = [
            pltpu.make_async_remote_copy(
                src_ref=moment_ref if s == 0 else mom_send_ref.at[s],
                dst_ref=mom_land_ref.at[s],
                send_sem=mom_send_sem.at[s], recv_sem=mom_recv_sem.at[s],
                device_id=(partner(s), bl), device_id_type=MESH,
            )
        ]
        for i in range(pieces):
            if s == 0:
                source = image_ref.at[partner(0) % 2 + i * 2]
            else:
                source = work_ref.at[s - 1, (partner(s) // 2**s) % 2 + 2 * i]
            copies.append(
                pltpu.make_async_remote_copy(
                    src_ref=source, dst_ref=land_ref.at[slot + i],
                    send_sem=send_sem.at[slot + i], recv_sem=recv_sem.at[slot + i],
                    device_id=(partner(s), bl), device_id_type=MESH,
                )
            )
        for copy in copies:
            copy.start()
        copies[0].wait()
        before = moment_ref[...] if s == 0 else mom_send_ref[s]
        mom_send_ref[s + 1] = before + mom_land_ref[s]
        for i in range(pieces):
            copies[1 + i].wait()
            if s == 0:
                own = image_ref[chan % 2 + i * 2]
            else:
                own = work_ref[s - 1, (chan // 2**s) % 2 + 2 * i]
            if s + 1 < steps:
                work_ref[s, i] = own + land_ref[slot + i]
            else:
                sum_ref[...] = own + land_ref[slot + i]
        slot += pieces

    copies = []
    for d in range(1, n_bl):
        copies.append(
            pltpu.make_async_remote_copy(
                src_ref=mom_send_ref.at[steps], dst_ref=bl_mom_ref.at[d],
                send_sem=blm_send.at[d], recv_sem=blm_recv.at[d],
                device_id=(chan, peer(d)), device_id_type=MESH,
            )
        )
        copies.append(
            pltpu.make_async_remote_copy(
                src_ref=sum_ref.at[peer(d)], dst_ref=bl_land_ref.at[d],
                send_sem=bl_send.at[d], recv_sem=bl_recv.at[d],
                device_id=(chan, peer(d)), device_id_type=MESH,
            )
        )
    for copy in copies:
        copy.start()
    moments = mom_send_ref[steps]
    images = sum_ref[bl]
    for d in range(1, n_bl):
        copies[2 * d - 2].wait()
        copies[2 * d - 1].wait()
        moments = moments + bl_mom_ref[d]
        images = images + bl_land_ref[d]
    solved = solve_taylor([moments[m : m + 1] for m in range(MOMENTS)], images)
    for k in range(TAYLOR):
        out_ref[k] = solved[k]


def reduce_solve(n_chan, n_bl, image, moment):
    chunks, taylor, rows, lanes = image.shape
    image = image.reshape(n_chan, n_bl, taylor, rows, lanes)
    vmem = pl.BlockSpec(memory_space=pltpu.VMEM)
    block = (n_bl, taylor, rows, lanes)
    steps = n_chan.bit_length() - 1
    dma = pltpu.SemaphoreType.DMA
    return pl.pallas_call(
        functools.partial(reduce_kernel, n_chan, n_bl),
        out_shape=jax.ShapeDtypeStruct((taylor, rows, lanes), jnp.float32),
        in_specs=[vmem, vmem],
        out_specs=vmem,
        scratch_shapes=[
            pltpu.VMEM((max(steps - 1, 1), n_chan // 2) + block, jnp.float32),
            pltpu.VMEM((n_chan - 1,) + block, jnp.float32),
            pltpu.VMEM(block, jnp.float32),
            pltpu.VMEM((steps + 1, 8, lanes), jnp.float32),
            pltpu.VMEM((steps, 8, lanes), jnp.float32),
            pltpu.VMEM((n_bl, taylor, rows, lanes), jnp.float32),
            pltpu.VMEM((n_bl, 8, lanes), jnp.float32),
            dma((n_chan - 1,)), dma((n_chan - 1,)), dma((steps,)), dma((steps,)),
            dma((n_bl,)), dma((n_bl,)), dma((n_bl,)), dma((n_bl,)),
        ],
        compiler_params=pltpu.CompilerParams(collective_id=0, has_side_effects=True),
        name="reduce_solve",
    )(image, moment)


def solution(mesh):
    n_chan = mesh.shape["chan"]
    n_bl = mesh.shape["bl"]

    def body(vis_value, vis_weight, kernel, tile_index, plane_index, chan_index, chan_offset, counts):
        image, moment = local_image(
            n_chan * n_bl, counts, chan_offset, vis_value[0, 0], vis_weight[0], kernel[0, 0],
            tile_index[0], plane_index[0], chan_index[0],
        )
        out = reduce_solve(n_chan, n_bl, image, moment)
        return out.reshape(TAYLOR, -1)

    in_specs = (
        P("chan", "bl", None, None),
        P("chan", "bl", None),
        P("chan", "bl", None, None),
        P("chan", "bl", None),
        P("chan", "bl", None),
        P("chan", "bl", None),
        P("chan", None),
        P("chan", "bl"),
    )
    out_specs = P(None, ("chan", "bl"))
    return jax.shard_map(body, mesh=mesh, in_specs=in_specs, out_specs=out_specs, check_vma=False)
```
